32 devices in a mesh: er: 2 (over x), ec: 4 (over z), dp: 4 (over y, core).
Axes of the slice: x: 2, y: 2, z: 4, core: 2. Of those that a mesh axis runs over, the one named last changes fastest.
Arguments:
- out_grad: bfloat16 [4, 512, 4096], P('dp', 'er', 'ec'), may hold values from -6 to 6
- route_probs: float32 [4, 512], P('dp', 'er'), may hold values from 0.1 to 1
- expert_ids: int32 [4, 512], P('dp', 'er'), may hold values from 0 to 1, as said below
- slot_ids: int32 [4, 512], P('dp', 'er'), may hold values from 0 to 143, as said below
- gate_pre: bfloat16 [4, 2, 288, 768], P('dp', 'er'), may hold values from -6 to 6
- up_act: bfloat16 [4, 2, 288, 768], P('dp', 'er'), may hold values from -6 to 6
- w_gate: bfloat16 [2, 4096, 768], P('er', 'ec'), may hold values from -0.09375 to 0.09375
- w_up: bfloat16 [2, 4096, 768], P('er', 'ec'), may hold values from -0.09375 to 0.09375
- w_down: bfloat16 [2, 768, 4096], P('er', None, 'ec'), may hold values from -0.21875 to 0.21875
Outputs:
- input_grad: bfloat16 [4, 512, 4096], P('dp', 'er', 'ec')
- down_grad: float32 [2, 768, 4096], P('er', 'dp', 'ec')
The draws below stay inside these ranges and needn't reach their ends.
Inputs may be any that keep to these rules, and one draw needn't show every extreme that they name: `expert_ids`: within each group of 256 tokens no expert is chosen by more than 144 tokens; in every replica some expert is chosen by exactly 144 tokens of every group of that replica. `slot_ids`: tokens of one group that chose the same expert have distinct slots.
All inputs are finite; a program needn't handle non-finite values.
Results may differ from the reference program's by a relative error of at most 0.015.
Values may be sent and summed in bfloat16 or wider, within the bound.
No kernel may reach another device: no remote copies, remote signals or barrier semaphores. Data moves between devices by JAX's collectives and lax.ppermute only.
A program may use at most 64 MiB of HBM per device.

```python
import jax
import jax.numpy as jnp
from jax import lax

D = 4096
H = 768
TOK = 256
C = 144
N_ER = 2
N_DP = 4


def route_table(key):

    def group_draw(replica, row_index):
        full_expert = jax.random.randint(jax.random.fold_in(jax.random.fold_in(key, 101), replica), (), 0, N_ER)
        group_key = jax.random.fold_in(jax.random.fold_in(key, 202), replica * N_ER + row_index)
        first_key, second_key = jax.random.split(group_key)
        ranking = jax.random.permutation(first_key, N_ER * C)
        slot_cells = jnp.arange(N_ER * C)
        scores = jnp.where(slot_cells // C == full_expert, ranking - N_ER * C, ranking)
        picked = jnp.argsort(scores, stable=True)[:TOK]
        picked = jax.random.permutation(second_key, picked)
        return (picked // C, picked % C)
    replicas = jnp.repeat(jnp.arange(N_DP), N_ER)
    row_values = jnp.tile(jnp.arange(N_ER), N_DP)
    chosen, placed = jax.vmap(group_draw)(replicas, row_values)
    return (chosen.reshape(N_DP, N_ER * TOK).astype(jnp.int32), placed.reshape(N_DP, N_ER * TOK).astype(jnp.int32))


def draw_expert_ids(key, part):
    return route_table(key)[0]


def draw_slot_ids(key, part):
    return route_table(key)[1]


def block_scale(own_key, shape, cuts, smallest, largest):
    loudness, own = 1.0, jax.random.fold_in(own_key, 6)
    for position, blocks in cuts:
        heights = jnp.exp(jax.random.uniform(jax.random.fold_in(own, position), (blocks,), jnp.float32, smallest / len(cuts), largest / len(cuts)))
        loudness = loudness * jnp.repeat(heights, shape[position] // blocks).reshape([-1 if axis == position else 1 for axis in range(len(shape))])
    return loudness


def normal_values(stream_key, shape, scale, bound, cuts=(), kind=jnp.bfloat16):
    array = jax.random.normal(stream_key, shape, jnp.float32) * scale
    if len(cuts) > 0:
        array = block_scale(stream_key, shape, cuts, -0.22, 0.18) * array
    return jnp.clip(array, min=-bound, max=bound).astype(kind)


def setup_inputs(seed: int = 0) -> dict:
    streams_of = jax.random.split(jax.random.key(seed), 10)
    out_grad = normal_values(streams_of[0], (N_DP, N_ER * TOK, D), 1.0, 6.0, ((0, 4), (1, 2), (2, 4)))
    route_probs = jnp.clip(0.1 + 0.9 * jax.random.uniform(streams_of[1], (N_DP, N_ER * TOK), jnp.float32) ** block_scale(streams_of[1], (N_DP, N_ER * TOK), ((0, 4), (1, 2)), -0.2, 0.2), 0.1, 1.0)
    expert_ids = draw_expert_ids(jax.random.fold_in(streams_of[9], 71), 0)
    slot_ids = draw_slot_ids(jax.random.fold_in(streams_of[9], 71), 0)
    gate_pre = normal_values(streams_of[4], (N_DP, N_ER, N_ER * C, H), 1.0, 6.0, ((0, 4), (1, 2)))
    up_act = normal_values(streams_of[5], (N_DP, N_ER, N_ER * C, H), 1.0, 6.0, ((0, 4), (1, 2)))
    w_gate = normal_values(streams_of[6], (N_ER, D, H), D ** -0.5, 0.09375, ((0, 2), (1, 4)))
    w_up = normal_values(streams_of[7], (N_ER, D, H), D ** -0.5, 0.09375, ((0, 2), (1, 4)))
    w_down = normal_values(streams_of[8], (N_ER, H, D), H ** -0.5, 0.21875, ((0, 2), (2, 4)))
    return {"out_grad": out_grad, "route_probs": route_probs, "expert_ids": expert_ids, "slot_ids": slot_ids, "gate_pre": gate_pre, "up_act": up_act, "w_gate": w_gate, "w_up": w_up, "w_down": w_down}


def reference(out_grad, route_probs, expert_ids, slot_ids, gate_pre, up_act, w_gate, w_up, w_down):
    slot_count = N_ER * C
    group_index = jnp.arange(N_ER * TOK, dtype=jnp.int32) // TOK

    def expert_step(pieces):
        slot_input, pre_rows, up_rows, gate_mat, up_mat, down_mat = pieces
        hid_grad = jnp.dot(slot_input, down_mat.T, preferred_element_type=jnp.float32)
        pre_float = pre_rows.astype(jnp.float32)
        up_float = up_rows.astype(jnp.float32)
        sigmoid = jax.nn.sigmoid(pre_float)
        gate_grad = (hid_grad * up_float * sigmoid * (1.0 + pre_float * (1.0 - sigmoid))).astype(jnp.bfloat16)
        up_grad = (hid_grad * pre_float * sigmoid).astype(jnp.bfloat16)
        hidden = (pre_float * sigmoid * up_float).astype(jnp.bfloat16)
        slot_grad = (jnp.dot(gate_grad, gate_mat.T, preferred_element_type=jnp.float32)
                     + jnp.dot(up_grad, up_mat.T, preferred_element_type=jnp.float32)).astype(jnp.bfloat16)
        weight_part = jnp.dot(hidden.T, slot_input, preferred_element_type=jnp.float32)
        return slot_grad, weight_part

    def replica(weight_total, inputs):
        grad_rows, prob_rows, expert_rows, slot_rows, pre_all, up_all = inputs
        scaled = (prob_rows[:, None] * grad_rows.astype(jnp.float32)).astype(jnp.bfloat16)
        target = (expert_rows * slot_count + group_index * C + slot_rows).astype(jnp.int32)
        placed = jnp.zeros((N_ER * slot_count, D), jnp.bfloat16).at[target].set(scaled)
        placed = placed.reshape(N_ER, slot_count, D)
        slot_grads, weight_parts = lax.map(expert_step, (placed, pre_all, up_all, w_gate, w_up, w_down))
        token_grads = slot_grads.reshape(N_ER * slot_count, D)[target]
        return weight_total + weight_parts, token_grads

    weight_total, input_grad = lax.scan(
        replica, jnp.zeros((N_ER, H, D), jnp.float32),
        (out_grad, route_probs, expert_ids, slot_ids, gate_pre, up_act))
    return input_grad, weight_total / N_DP
```

```python
import jax
import jax.numpy as jnp
from jax import lax
from jax.sharding import PartitionSpec as P


def shift(x, axis, step):
    n = lax.axis_size(axis)
    return lax.ppermute(x, axis, [(j, (j + step) % n) for j in range(n)])


def block_grid(rows, cols, n):
    across = 2 if n % 2 == 0 and rows % (n // 2) == 0 and cols % 256 == 0 else 1
    return n // across, across


def take_block(x, index, grid):
    down, across = grid
    rows, cols = x.shape[0] // down, x.shape[1] // across
    return lax.dynamic_slice(x, (index // across * rows, index % across * cols), (rows, cols))


def sum_over_ec(partial_value):
    n = lax.axis_size("ec")
    me = lax.axis_index("ec")
    grid = block_grid(*partial_value.shape, n)
    rounded = partial_value.astype(jnp.bfloat16)
    pieces = [shift(take_block(rounded, (me + s) % n, grid), "ec", s) for s in range(1, n)]
    return pieces, take_block(partial_value, me, grid)


def finish_sum(pieces, own):
    total = own.astype(jnp.float32)
    for piece in pieces:
        total = total + piece.astype(jnp.float32)
    return total.astype(jnp.bfloat16)


def gather_over_ec(block, shape):
    n = lax.axis_size("ec")
    me = lax.axis_index("ec")
    grid = block_grid(*shape, n)
    rows, cols = block.shape
    whole = jnp.zeros(shape, jnp.bfloat16)
    for s in range(n):
        arrived = block if s == 0 else shift(block, "ec", -s)
        index = (me + s) % n
        whole = lax.dynamic_update_slice(whole, arrived, (index // grid[1] * rows, index % grid[1] * cols))
    return whole


def swiglu_grads(hid_grad, pre_rows, up_rows):
    hid_float = hid_grad.astype(jnp.float32)
    pre_float = pre_rows.astype(jnp.float32)
    up_float = up_rows.astype(jnp.float32)
    sigmoid = jax.nn.sigmoid(pre_float)
    gate_grad = (hid_float * up_float * sigmoid * (1.0 + pre_float * (1.0 - sigmoid))).astype(jnp.bfloat16)
    up_grad = (hid_float * pre_float * sigmoid).astype(jnp.bfloat16)
    return gate_grad, up_grad


def matmul_nt(a, b):
    return lax.dot_general(a, b, (((1,), (1,)), ((), ())), preferred_element_type=jnp.float32)


def matmul_tn(a, b):
    return lax.dot_general(a, b, (((0,), (0,)), ((), ())), preferred_element_type=jnp.float32)


def scatter_sum_over_dp(total):
    n = lax.axis_size("dp")
    if n & (n - 1):
        return lax.psum_scatter(total, "dp", scatter_dimension=0, tiled=True)
    me = lax.axis_index("dp")
    rows, cols = total.shape
    block = rows // n
    total = total.reshape(n, block, cols)
    bit = 1
    while bit < n:
        pairs = total.reshape(total.shape[0] // 2, 2, block, cols)
        mine = (me // bit) % 2
        sent = lax.dynamic_slice_in_dim(pairs, 1 - mine, 1, 1)[:, 0].astype(jnp.bfloat16)
        kept = lax.dynamic_slice_in_dim(pairs, mine, 1, 1)[:, 0]
        got = lax.ppermute(sent, "dp", [(j, j ^ bit) for j in range(n)])
        total = kept + got.astype(jnp.float32)
        bit *= 2
    return total[0]


def body(out_grad, route_probs, expert_ids, slot_ids, gate_pre, up_act, w_gate, w_up, w_down):
    tokens = out_grad[0]
    experts = lax.axis_size("er")
    me = lax.axis_index("er")
    capacity = gate_pre.shape[2] // experts
    slot_count = experts * capacity
    hidden_size = gate_pre.shape[3]
    position = (expert_ids[0] - me) % experts * capacity + slot_ids[0]
    chosen = (lax.broadcasted_iota(jnp.int32, (slot_count, tokens.shape[0]), 0) == position[None, :]).astype(
        jnp.bfloat16
    )
    scaled = (route_probs[0][:, None] * tokens.astype(jnp.float32)).astype(jnp.bfloat16)
    outgoing = lax.dot_general(chosen, scaled, (((1,), (0,)), ((), ())), preferred_element_type=jnp.float32).astype(
        jnp.bfloat16
    )
    own_rows = outgoing[:capacity]
    far_rows = jnp.concatenate(
        [shift(outgoing[s * capacity : (s + 1) * capacity], "er", s) for s in range(1, experts)], 0
    )

    def group_rows(x, s):
        return lax.dynamic_slice_in_dim(x, (me - s) % experts * capacity, capacity, 0)

    def far_groups(x):
        return jnp.concatenate([group_rows(x, s) for s in range(1, experts)], 0)

    pre_own, up_own = group_rows(gate_pre[0, 0], 0), group_rows(up_act[0, 0], 0)
    pre_far, up_far = far_groups(gate_pre[0, 0]), far_groups(up_act[0, 0])

    own_pieces, own_block = sum_over_ec(matmul_nt(own_rows, w_down[0]))
    far_pieces, far_block = sum_over_ec(matmul_nt(far_rows, w_down[0]))
    hid_far = gather_over_ec(finish_sum(far_pieces, far_block), (far_rows.shape[0], hidden_size))
    hid_own = gather_over_ec(finish_sum(own_pieces, own_block), (own_rows.shape[0], hidden_size))

    def slot_grads(hid_grad, pre_rows, up_rows):
        gate_grad, up_grad = swiglu_grads(hid_grad, pre_rows, up_rows)
        return (matmul_nt(gate_grad, w_gate[0]) + matmul_nt(up_grad, w_up[0])).astype(jnp.bfloat16)

    grad_far = slot_grads(hid_far, pre_far, up_far)
    grad_own = slot_grads(hid_own, pre_own, up_own)
    back = [shift(grad_far[(s - 1) * capacity : s * capacity], "er", -s) for s in range(1, experts)]

    def hidden_of(pre_rows, up_rows):
        pre_float = pre_rows.astype(jnp.float32)
        return (pre_float * jax.nn.sigmoid(pre_float) * up_rows.astype(jnp.float32)).astype(jnp.bfloat16)

    weight_part = matmul_tn(hidden_of(pre_own, up_own), own_rows) + matmul_tn(hidden_of(pre_far, up_far), far_rows)
    down_part = scatter_sum_over_dp(weight_part) / lax.axis_size("dp")

    input_grad = matmul_tn(chosen, jnp.concatenate([grad_own] + back, 0)).astype(jnp.bfloat16)
    return (input_grad[None], down_part[None])


def solution(mesh):
    in_specs = (
        P("dp", "er", "ec"),
        P("dp", "er"),
        P("dp", "er"),
        P("dp", "er"),
        P("dp", "er", None, None),
        P("dp", "er", None, None),
        P("er", "ec", None),
        P("er", "ec", None),
        P("er", None, "ec"),
    )
    out_specs = (P("dp", "er", "ec"), P("er", "dp", "ec"))
    return jax.shard_map(body, mesh=mesh, in_specs=in_specs, out_specs=out_specs, check_vma=False)
```

```python
import functools

import jax
import jax.numpy as jnp
from jax import lax
from jax.experimental import pallas as pl
from jax.experimental.pallas import tpu as pltpu
from jax.sharding import PartitionSpec as P


VMEM_LIMIT = 12 * 1024 * 1024


def shift(x, axis, step):
    n = lax.axis_size(axis)
    return lax.ppermute(x, axis, [(j, (j + step) % n) for j in range(n)])


def swap(x, axis, bit):
    return lax.ppermute(x, axis, [(j, j ^ bit) for j in range(lax.axis_size(axis))])


def wrap(x, n):
    return jnp.where(x < 0, x + n, x)


def matmul_nt(a, b):
    return lax.dot_general(a, b, (((1,), (1,)), ((), ())), preferred_element_type=jnp.float32)


def matmul_tn(a, b):
    return lax.dot_general(a, b, (((0,), (0,)), ((), ())), preferred_element_type=jnp.float32)


def call(kernel, outs, *args, stored=(), scratch=(), to_hbm=False, flops=1e6):
    vmem = pl.BlockSpec(memory_space=pltpu.VMEM)
    hbm = pl.BlockSpec(memory_space=pltpu.HBM)
    out_type = pltpu.HBM if to_hbm else pltpu.VMEM
    result = pl.pallas_call(
        kernel,
        out_shape=[out_type(shape, dtype) for shape, dtype in outs],
        in_specs=[vmem] * len(args) + [hbm] * len(stored),
        out_specs=[hbm if to_hbm else vmem] * len(outs),
        scratch_shapes=list(scratch),
        compiler_params=pltpu.CompilerParams(vmem_limit_bytes=VMEM_LIMIT),
        cost_estimate=pl.CostEstimate(flops=int(flops), transcendentals=0, bytes_accessed=1024),
    )(*args, *(pltpu.with_memory_space_constraint(x, pltpu.HBM) for x in stored))
    return result if len(outs) > 1 else result[0]


def load(sources, targets, sems):
    copies = [pltpu.make_async_copy(x, y, sems.at[i]) for i, (x, y) in enumerate(zip(sources, targets))]
    for copy in copies:
        copy.start()
    return copies


def half_index():
    me = lax.axis_index("ec")
    return lax.shift_right_logical(me + 1, 1) & 1


def one_hot(position, count):
    hit = lax.broadcasted_iota(jnp.int32, (count, position.shape[1]), 0) == position
    return hit, jnp.where(hit, 1.0, 0.0).astype(jnp.bfloat16)


def dispatch_kernel(ids, slots, probs, tokens, down, own, far, position, weights, v_ids, v_slots, v_probs, v_tokens, sems):
    capacity = own.shape[0]
    count = capacity + far.shape[0]
    copies = load((ids, slots, probs, tokens, down), (v_ids, v_slots, v_probs, v_tokens, weights), sems)
    for copy in copies[:4]:
        copy.wait()
    where = wrap(v_ids[...] - lax.axis_index("er"), count // capacity) * capacity + v_slots[...]
    position[...] = where
    hit, chosen = one_hot(where, count)
    prob = jnp.sum(jnp.where(hit, v_probs[...], 0.0), axis=1, keepdims=True)
    rows = lax.dot_general(chosen, v_tokens[...], (((1,), (0,)), ((), ())), preferred_element_type=jnp.float32)
    scaled = (prob * rows).astype(jnp.bfloat16)
    own[...] = scaled[:capacity]
    far[...] = scaled[capacity:]
    copies[4].wait()


def hidden_kernel(rows, weights, sent, kept):
    half = kept.shape[1]
    mine = half_index()
    value = rows[...]
    sent[...] = matmul_nt(value, weights[pl.ds(pl.multiple_of((1 - mine) * half, half), half), :]).astype(
        jnp.bfloat16
    )
    kept[...] = matmul_nt(value, weights[pl.ds(pl.multiple_of(mine * half, half), half), :])


def pair_kernel(kept, got, sent):
    sent[...] = (kept[...] + got[...].astype(jnp.float32)).astype(jnp.bfloat16)


def across_kernel(kept, got, more, total):
    total[...] = (kept[...] + got[...].astype(jnp.float32) + more[...].astype(jnp.float32)).astype(jnp.bfloat16)


def prepare_kernel(pre, up, gate, lift, hidden, by_gate, by_up, w_gate, w_up, v_pre, v_up, sems):
    copies = load((pre, up, gate, lift), (v_pre, v_up, w_gate, w_up), sems)
    for copy in copies[:2]:
        copy.wait()
    groups, capacity, _ = hidden.shape
    for step in range(groups):
        start = pl.multiple_of(wrap(lax.axis_index("er") - step, groups) * capacity, capacity)
        a = v_pre[pl.ds(start, capacity), :].astype(jnp.float32)
        u = v_up[pl.ds(start, capacity), :].astype(jnp.float32)
        s = jax.nn.sigmoid(a)
        hidden[step] = (a * s * u).astype(jnp.bfloat16)
        by_gate[step] = u * s * (1.0 + a * (1.0 - s))
        by_up[step] = a * s
    for copy in copies[2:]:
        copy.wait()


def grads_kernel(step, kept, other, by_gate, by_up, w_gate, w_up, out):
    half = kept.shape[1]
    mine = half_index()
    total = None
    for h in range(2):
        part = slice(h * half, (h + 1) * half)
        hid = jnp.where(mine == h, kept[...], other[...]).astype(jnp.float32)
        gate_grad = (hid * by_gate[step, :, part]).astype(jnp.bfloat16)
        up_grad = (hid * by_up[step, :, part]).astype(jnp.bfloat16)
        value = matmul_nt(gate_grad, w_gate[:, part]) + matmul_nt(up_grad, w_up[:, part])
        total = value if total is None else total + value
    out[...] = total.astype(jnp.bfloat16)


def weight_kernel(own, far, hidden, sent, kept):
    groups, capacity, _ = hidden.shape
    total = None
    for step in range(groups):
        rows = own[...] if step == 0 else far[(step - 1) * capacity : step * capacity]
        value = matmul_tn(hidden[step], rows)
        total = value if total is None else total + value
    pairs, block, _ = sent.shape
    for c in range(2):

        @pl.when((lax.axis_index("dp") & 1) == c)
        def _():
            for y in range(pairs):
                low, high = total[2 * y * block : (2 * y + 1) * block], total[(2 * y + 1) * block : (2 * y + 2) * block]
                kept[y] = high if c else low
                sent[y] = (low if c else high).astype(jnp.bfloat16)


def halve_kernel(bit, kept, got, sent, left):
    mine = lax.shift_right_logical(lax.axis_index("dp"), bit) & 1
    pairs = left.shape[0]
    for p in range(pairs):
        sent[p] = (kept[2 * p + 1 - mine] + got[2 * p + 1 - mine].astype(jnp.float32)).astype(jnp.bfloat16)
        left[p] = kept[2 * p + mine] + got[2 * p + mine].astype(jnp.float32)


def mean_kernel(replicas, kept, got, out, staged, sem):
    staged[...] = (kept[...] + got[...].astype(jnp.float32)) / replicas
    copy = pltpu.make_async_copy(staged, out, sem)
    copy.start()
    copy.wait()


def combine_kernel(pieces, position, own, back, out, staged, sems):
    capacity, count = own.shape[0], own.shape[0] + back.shape[0]
    _, chosen = one_hot(position[...], count)
    size = staged.shape[0] // pieces
    copies = []
    for i in range(pieces):
        part = slice(i * size, (i + 1) * size)
        value = matmul_tn(chosen[:capacity, part], own[...]) + matmul_tn(chosen[capacity:, part], back[...])
        staged[part] = value.astype(jnp.bfloat16)
        copies.append(pltpu.make_async_copy(staged.at[part], out.at[part], sems.at[i]))
        copies[-1].start()
    for copy in copies:
        copy.wait()


def start_sum(rows, weights):
    count, half = rows.shape[0], weights.shape[0] // 2
    flops = 4 * count * half * rows.shape[1]
    sent, kept = call(
        hidden_kernel, [((count, half), jnp.bfloat16), ((count, half), jnp.float32)], rows, weights, flops=flops
    )
    got = swap(sent, "ec", 1)
    sent = call(pair_kernel, [(sent.shape, jnp.bfloat16)], kept, got)
    more = swap(sent, "ec", 3)
    total = call(across_kernel, [(sent.shape, jnp.bfloat16)], kept, got, more)
    return total, swap(total, "ec", 1)


def fast_body(out_grad, route_probs, expert_ids, slot_ids, gate_pre, up_act, w_gate, w_up, w_down):
    tokens = out_grad[0]
    experts = lax.axis_size("er")
    replicas = lax.axis_size("dp")
    pre, up = gate_pre[0, 0], up_act[0, 0]
    capacity = pre.shape[0] // experts
    slot_count = experts * capacity
    count, width = tokens.shape
    hidden_size = pre.shape[1]
    bf16, f32, i32 = jnp.bfloat16, jnp.float32, jnp.int32
    own, far, position, down = call(
        dispatch_kernel,
        [
            ((capacity, width), bf16),
            ((slot_count - capacity, width), bf16),
            ((1, count), i32),
            ((hidden_size, width), bf16),
        ],
        stored=(expert_ids, slot_ids, route_probs, tokens, w_down[0]),
        scratch=[
            pltpu.VMEM((1, count), i32),
            pltpu.VMEM((1, count), i32),
            pltpu.VMEM((1, count), f32),
            pltpu.VMEM((count, width), bf16),
            pltpu.SemaphoreType.DMA((5,)),
        ],
        flops=2 * slot_count * tokens.size,
    )
    far = [shift(far[(s - 1) * capacity : s * capacity], "er", s) for s in range(1, experts)]
    rows = (experts, capacity, hidden_size)
    hidden, by_gate, by_up, gate, lift = call(
        prepare_kernel,
        [(rows, bf16), (rows, f32), (rows, f32), ((width, hidden_size), bf16), ((width, hidden_size), bf16)],
        stored=(pre, up, w_gate[0], w_up[0]),
        scratch=[pltpu.VMEM(pre.shape, bf16), pltpu.VMEM(pre.shape, bf16), pltpu.SemaphoreType.DMA((4,))],
        flops=1e9,
    )
    own_sum = start_sum(own, down)
    far_sums = [start_sum(x, down) for x in far]

    block = hidden_size // replicas
    sent, kept = call(
        weight_kernel,
        [((replicas // 2, block, width), bf16), ((replicas // 2, block, width), f32)],
        own,
        jnp.concatenate(far, 0) if len(far) > 1 else far[0],
        hidden,
        flops=2 * slot_count * hidden_size * width,
    )
    bit = 0
    while True:
        got = swap(sent, "dp", 1 << bit)
        if kept.shape[0] == 1:
            break
        bit += 1
        shape = (kept.shape[0] // 2, block, width)
        sent, kept = call(functools.partial(halve_kernel, bit), [(shape, bf16), (shape, f32)], kept, got, flops=1e8)
    down_part = call(
        functools.partial(mean_kernel, replicas),
        [(kept.shape, f32)],
        kept,
        got,
        scratch=[pltpu.VMEM(kept.shape, f32), pltpu.SemaphoreType.DMA],
        to_hbm=True,
    )

    def slot_grads(total, step):
        flops = 4 * capacity * hidden_size * width
        kernel = functools.partial(grads_kernel, step)
        return call(kernel, [((capacity, width), bf16)], *total, by_gate, by_up, gate, lift, flops=flops)

    grad_own = slot_grads(own_sum, 0)
    back = [shift(slot_grads(far_sums[s - 1], s), "er", -s) for s in range(1, experts)]
    pieces = 4 if count % 64 == 0 else 1
    input_grad = call(
        functools.partial(combine_kernel, pieces),
        [((count, width), bf16)],
        position,
        grad_own,
        jnp.concatenate(back, 0) if len(back) > 1 else back[0],
        scratch=[pltpu.VMEM((count, width), bf16), pltpu.SemaphoreType.DMA((pieces,))],
        to_hbm=True,
        flops=2 * slot_count * tokens.size,
    )
    return (input_grad[None], down_part)


def solution(mesh):
    in_specs = (
        P("dp", "er", "ec"),
        P("dp", "er"),
        P("dp", "er"),
        P("dp", "er"),
        P("dp", "er", None, None),
        P("dp", "er", None, None),
        P("er", "ec", None),
        P("er", "ec", None),
        P("er", None, "ec"),
    )
    out_specs = (P("dp", "er", "ec"), P("er", "dp", "ec"))
    return jax.shard_map(fast_body, mesh=mesh, in_specs=in_specs, out_specs=out_specs, check_vma=False)
```

```python
import functools

import jax
import jax.numpy as jnp
from jax import lax
from jax.experimental import pallas as pl
from jax.experimental.pallas import tpu as pltpu
from jax.sharding import PartitionSpec as P


VMEM_LIMIT = 12 * 1024 * 1024


def shift(x, axis, step):
    n = lax.axis_size(axis)
    return lax.ppermute(x, axis, [(j, (j + step) % n) for j in range(n)])


def swap(x, axis, bit):
    return lax.ppermute(x, axis, [(j, j ^ bit) for j in range(lax.axis_size(axis))])


def wrap(x, n):
    return jnp.where(x < 0, x + n, x)


def matmul_nt(a, b):
    return lax.dot_general(a, b, (((1,), (1,)), ((), ())), preferred_element_type=jnp.float32)


def matmul_tn(a, b):
    return lax.dot_general(a, b, (((0,), (0,)), ((), ())), preferred_element_type=jnp.float32)


def call(kernel, outs, *args, stored=(), scratch=(), to_hbm=False, flops=1e6):
    vmem = pl.BlockSpec(memory_space=pltpu.VMEM)
    hbm = pl.BlockSpec(memory_space=pltpu.HBM)
    out_type = pltpu.HBM if to_hbm else pltpu.VMEM
    result = pl.pallas_call(
        kernel,
        out_shape=[out_type(shape, dtype) for shape, dtype in outs],
        in_specs=[vmem] * len(args) + [hbm] * len(stored),
        out_specs=[hbm if to_hbm else vmem] * len(outs),
        scratch_shapes=list(scratch),
        compiler_params=pltpu.CompilerParams(vmem_limit_bytes=VMEM_LIMIT),
        cost_estimate=pl.CostEstimate(flops=int(flops), transcendentals=0, bytes_accessed=1024),
    )(*args, *(pltpu.with_memory_space_constraint(x, pltpu.HBM) for x in stored))
    return result if len(outs) > 1 else result[0]


def load(sources, targets, sems):
    copies = [pltpu.make_async_copy(x, y, sems.at[i]) for i, (x, y) in enumerate(zip(sources, targets))]
    for copy in copies:
        copy.start()
    return copies


def half_index(bit):
    return lax.shift_right_logical(lax.axis_index("ec"), bit) & 1


def one_hot(position, count):
    hit = lax.broadcasted_iota(jnp.int32, (count, position.shape[1]), 0) == position
    return hit, jnp.where(hit, 1.0, 0.0).astype(jnp.bfloat16)


def dispatch_kernel(ids, slots, probs, tokens, down, *refs):
    *rows_out, position, weights, v_ids, v_slots, v_probs, v_tokens, sems = refs
    count = sum(out.shape[0] for out in rows_out)
    copies = load((ids, slots, probs, tokens, down), (v_ids, v_slots, v_probs, v_tokens, weights), sems)
    for copy in copies[:4]:
        copy.wait()
    capacity = rows_out[0].shape[0]
    where = wrap(v_ids[...] - lax.axis_index("er"), count // capacity) * capacity + v_slots[...]
    position[...] = where
    hit, chosen = one_hot(where, count)
    prob = jnp.sum(jnp.where(hit, v_probs[...], 0.0), axis=1, keepdims=True)
    rows = lax.dot_general(chosen, v_tokens[...], (((1,), (0,)), ((), ())), preferred_element_type=jnp.float32)
    scaled = prob * rows
    low = 0
    for out in rows_out:
        out[...] = scaled[low : low + out.shape[0]].astype(jnp.bfloat16)
        low += out.shape[0]
    copies[4].wait()


def hidden_kernel(bit, other, rows, weights, *outs):
    half = outs[0].shape[1]
    which = 1 - half_index(bit) if other else half_index(bit)
    value = matmul_nt(rows[...], weights[pl.ds(pl.multiple_of(which * half, half), half), :])
    low = 0
    for out in outs:
        out[...] = value[low : low + out.shape[0]].astype(out.dtype)
        low += out.shape[0]


def pair_kernel(kept, got, sent, total):
    value = kept[...] + got[...].astype(jnp.float32)
    total[...] = value
    sent[...] = value.astype(jnp.bfloat16)


def across_kernel(kept, got, *totals):
    value = kept[...] + got[...].astype(jnp.float32)
    low = 0
    for total in totals:
        total[...] = value[low : low + total.shape[0]].astype(jnp.bfloat16)
        low += total.shape[0]


def prepare_kernel(pre, up, gate, lift, *refs):
    *hidden, by_gate, by_up, both, v_pre, v_up, sems = refs
    half = both.shape[2] // 2
    pairs = [(pre, v_pre), (up, v_up)]
    for h in range(2):
        for k, weights in enumerate((gate, lift)):
            pairs.append((weights.at[:, h * half : (h + 1) * half], both.at[h, :, k * half : (k + 1) * half]))
    copies = load(*zip(*pairs), sems)
    for copy in copies[:2]:
        copy.wait()
    groups, capacity, _ = by_gate.shape
    outs = iter(hidden)
    for step in range(groups):
        start = pl.multiple_of(wrap(lax.axis_index("er") - step, groups) * capacity, capacity)
        a = v_pre[pl.ds(start, capacity), :].astype(jnp.float32)
        u = v_up[pl.ds(start, capacity), :].astype(jnp.float32)
        s = jax.nn.sigmoid(a)
        value = a * s * u
        low = 0
        while low < capacity:
            out = next(outs)
            out[...] = value[low : low + out.shape[0]].astype(jnp.bfloat16)
            low += out.shape[0]
        by_gate[step] = u * s * (1.0 + a * (1.0 - s))
        by_up[step] = a * s
    for copy in copies[2:]:
        copy.wait()


def half_grads(step, low, hid, which, by_gate, by_up, both):
    half = hid[0].shape[1]
    rows = slice(low, low + sum(x.shape[0] for x in hid))
    part = pl.ds(pl.multiple_of(which * half, half), half)
    value = jnp.concatenate([x[...].astype(jnp.float32) for x in hid], 0)
    gate_grad = (value * by_gate[step, rows, part]).astype(jnp.bfloat16)
    up_grad = (value * by_up[step, rows, part]).astype(jnp.bfloat16)
    return matmul_nt(jnp.concatenate([gate_grad, up_grad], 1), both[which])


def first_grads_kernel(bit, step, *refs):
    *kept, by_gate, by_up, both, out = refs
    out[...] = half_grads(step, 0, kept, half_index(bit), by_gate, by_up, both)


def last_grads_kernel(bit, step, low, other, first, by_gate, by_up, both, out):
    value = half_grads(step, low, [other], 1 - half_index(bit), by_gate, by_up, both)
    out[...] = (first[low : low + out.shape[0]] + value).astype(jnp.bfloat16)


def grads_kernel(bit, step, kept, other, by_gate, by_up, both, out):
    mine = half_index(bit)
    value = half_grads(step, 0, [kept], mine, by_gate, by_up, both)
    value = value + half_grads(step, 0, [other], 1 - mine, by_gate, by_up, both)
    out[...] = value.astype(jnp.bfloat16)


def weight_kernel(*refs):
    *pairs_in, sent, kept = refs
    chunks = len(pairs_in) // 2
    total = None
    for rows, hidden in zip(pairs_in[:chunks], pairs_in[chunks:]):
        value = matmul_tn(hidden[...], rows[...])
        total = value if total is None else total + value
    pairs, block, _ = sent.shape
    for c in range(2):

        @pl.when((lax.axis_index("dp") & 1) == c)
        def _():
            for y in range(pairs):
                low, high = total[2 * y * block : (2 * y + 1) * block], total[(2 * y + 1) * block : (2 * y + 2) * block]
                kept[y] = high if c else low
                sent[y] = (low if c else high).astype(jnp.bfloat16)


def halve_kernel(bit, kept, got, sent, left):
    mine = lax.shift_right_logical(lax.axis_index("dp"), bit) & 1
    pairs = left.shape[0]
    for p in range(pairs):
        sent[p] = (kept[2 * p + 1 - mine] + got[2 * p + 1 - mine].astype(jnp.float32)).astype(jnp.bfloat16)
        left[p] = kept[2 * p + mine] + got[2 * p + mine].astype(jnp.float32)


def mean_kernel(replicas, kept, got, out, staged, sem):
    staged[...] = (kept[...] + got[...].astype(jnp.float32)) / replicas
    copy = pltpu.make_async_copy(staged, out, sem)
    copy.start()
    copy.wait()


def token_rows(position, parts, low):
    total = None
    for part in parts:
        _, chosen = one_hot(position - low, part.shape[0])
        value = matmul_tn(chosen, part[...])
        total = value if total is None else total + value
        low += part.shape[0]
    return total


def combine_kernel(position, *refs):
    *parts, out = refs
    out[...] = token_rows(position[...], parts, 0).astype(jnp.bfloat16)


def finish_kernel(pieces, low, position, part, others, out, staged, sems):
    size = staged.shape[0] // pieces
    copies = []
    for i in range(pieces):
        span = slice(i * size, (i + 1) * size)
        value = token_rows(position[:, span], [part], low) + others[span].astype(jnp.float32)
        staged[span] = value.astype(jnp.bfloat16)
        copies.append(pltpu.make_async_copy(staged.at[span], out.at[span], sems.at[i]))
        copies[-1].start()
    for copy in copies:
        copy.wait()


def sum_over_ec(rows, weights, bits, cuts):
    half = weights.shape[0] // 2
    flops = 2 * rows.shape[0] * half * rows.shape[1]
    shape = (rows.shape[0], half)
    bf16, f32 = jnp.bfloat16, jnp.float32
    sent = call(functools.partial(hidden_kernel, bits[0], True), [(shape, bf16)], rows, weights, flops=flops)
    kept = call(functools.partial(hidden_kernel, bits[0], False), [(shape, f32)], rows, weights, flops=flops)
    got = swap(sent, "ec", 1 << bits[0])
    pair, mine = call(pair_kernel, [(shape, bf16), (shape, f32)], kept, got)
    more = swap(pair, "ec", 1 << bits[1])
    totals = call(across_kernel, [((n, half), bf16) for n in cuts], mine, more)
    totals = list(totals) if len(cuts) > 1 else [totals]
    return totals, [swap(x, "ec", 1 << bits[0]) for x in totals]


def fast_body(out_grad, route_probs, expert_ids, slot_ids, gate_pre, up_act, w_gate, w_up, w_down):
    tokens = out_grad[0]
    experts = lax.axis_size("er")
    replicas = lax.axis_size("dp")
    pre, up = gate_pre[0, 0], up_act[0, 0]
    capacity = pre.shape[0] // experts
    slot_count = experts * capacity
    count, width = tokens.shape
    hidden_size = pre.shape[1]
    bf16, f32, i32 = jnp.bfloat16, jnp.float32, jnp.int32
    cuts = 1
    chunks = [(0, 0, capacity)]
    for step in range(1, experts):
        chunks += [(step, i * capacity // cuts, capacity // cuts) for i in range(cuts)]
    *outgoing, position, down = call(
        dispatch_kernel,
        [((n, width), bf16) for _, _, n in chunks] + [((1, count), i32), ((hidden_size, width), bf16)],
        stored=(expert_ids, slot_ids, route_probs, tokens, w_down[0]),
        scratch=[
            pltpu.VMEM((1, count), i32),
            pltpu.VMEM((1, count), i32),
            pltpu.VMEM((1, count), f32),
            pltpu.VMEM((count, width), bf16),
            pltpu.SemaphoreType.DMA((5,)),
        ],
        flops=2 * slot_count * tokens.size,
    )
    arrived = [shift(x, "er", step) if i else x for i, (x, (step, _, _)) in enumerate(zip(outgoing, chunks))]
    factor = ((experts, capacity, hidden_size), f32)
    *hidden, by_gate, by_up, both = call(
        prepare_kernel,
        [((n, hidden_size), bf16) for _, _, n in chunks] + [factor, factor, ((2, width, hidden_size), bf16)],
        stored=(pre, up, w_gate[0], w_up[0]),
        scratch=[pltpu.VMEM(pre.shape, bf16), pltpu.VMEM(pre.shape, bf16), pltpu.SemaphoreType.DMA((6,))],
        flops=1e9,
    )
    cuts = [capacity // 2, capacity // 2] if experts == 2 and capacity % 16 == 0 else [capacity]
    own_bits = far_bits = (0, 1)
    sums = [sum_over_ec(arrived[step], down, far_bits if step else own_bits, cuts if step else [capacity]) for step in range(experts)]

    block = hidden_size // replicas
    sent, kept = call(
        weight_kernel,
        [((replicas // 2, block, width), bf16), ((replicas // 2, block, width), f32)],
        *arrived,
        *hidden,
        flops=2 * slot_count * hidden_size * width,
    )
    bit = 0
    while True:
        got = swap(sent, "dp", 1 << bit)
        if kept.shape[0] == 1:
            break
        bit += 1
        shape = (kept.shape[0] // 2, block, width)
        sent, kept = call(functools.partial(halve_kernel, bit), [(shape, bf16), (shape, f32)], kept, got, flops=1e8)
    down_part = call(
        functools.partial(mean_kernel, replicas),
        [(kept.shape, f32)],
        kept,
        got,
        scratch=[pltpu.VMEM(kept.shape, f32), pltpu.SemaphoreType.DMA],
        to_hbm=True,
    )

    factors = (by_gate, by_up, both)
    flops = 4 * capacity * hidden_size * width
    outs = [((capacity, width), bf16)]
    own_grad = call(functools.partial(grads_kernel, own_bits[0], 0), outs, *sums[0][0], *sums[0][1], *factors, flops=flops)
    parts = [own_grad]
    for step in range(1, experts):
        kept, other = sums[step]
        kernel = functools.partial(first_grads_kernel, far_bits[0], step)
        first = call(kernel, [((capacity, width), f32)], *kept, *factors, flops=flops // 2)
        low = 0
        for rows in other:
            n = rows.shape[0]
            kernel = functools.partial(last_grads_kernel, far_bits[0], step, low)
            grads = call(kernel, [((n, width), bf16)], rows, first, *factors, flops=flops // 2)
            parts.append(shift(grads, "er", -step))
            low += n

    *parts, last = parts
    flops = 2 * slot_count * tokens.size
    others = call(combine_kernel, [((count, width), bf16)], position, *parts, flops=flops)
    pieces = 4 if count % 256 == 0 else 1
    input_grad = call(
        functools.partial(finish_kernel, pieces, slot_count - last.shape[0]),
        [((count, width), bf16)],
        position,
        last,
        others,
        scratch=[pltpu.VMEM((count, width), bf16), pltpu.SemaphoreType.DMA((pieces,))],
        to_hbm=True,
        flops=flops,
    )
    return (input_grad[None], down_part)


def solution(mesh):
    in_specs = (
        P("dp", "er", "ec"),
        P("dp", "er"),
        P("dp", "er"),
        P("dp", "er"),
        P("dp", "er", None, None),
        P("dp", "er", None, None),
        P("er", "ec", None),
        P("er", "ec", None),
        P("er", None, "ec"),
    )
    out_specs = (P("dp", "er", "ec"), P("er", "dp", "ec"))
    return jax.shard_map(fast_body, mesh=mesh, in_specs=in_specs, out_specs=out_specs, check_vma=False)
```
